512 devices in a mesh: dp: 64 (over y, z_lo, core), inner: 8 (over z_hi, x).
Axes of the slice: x: 4, y: 4, z: 16 (z_hi: 2, z_lo: 8; z = z_hi * 8 + z_lo), core: 2. Of those that a mesh axis runs over, the one named last changes fastest.
Arguments:
- inputs: bfloat16 [512, 32, 32, 256], P(('dp', 'inner')), may hold values from -24 to 24
- cotangent: bfloat16 [512, 32, 32, 256], P(('dp', 'inner')), may hold values from -24 to 24
- kernel_taps: float32 [9, 256, 256], P(None, 'dp', 'inner'), may hold values from -1 to 1
Outputs:
- new_taps: float32 [9, 256, 256], P(None, 'dp', 'inner')
The draws below stay inside these ranges and needn't reach their ends.
All inputs are finite; a program needn't handle non-finite values.
Results may differ from the reference program's by a relative error of at most 0.0003.
Values sent between devices are 32-bit elements; how exact they have to be, the bound alone decides.
A program may use at most 64 MiB of HBM per device.

```python
import math
import jax
import jax.numpy as jnp
from jax import lax

CHANNELS = 256
MAPSIDE = 32
BATCH = 512
FREQS = 544
N_DP = 64
N_INNER = 8


def scaled_field(key, salt):
    field_key, scale_key = jax.random.split(jax.random.fold_in(key, salt))
    shape = (BATCH, MAPSIDE, MAPSIDE, CHANNELS)
    position = jnp.arange(CHANNELS, dtype=jnp.float32) / CHANNELS
    rough = jax.random.uniform(scale_key, (CHANNELS,), jnp.float32, 0.8, 1.25)
    values = jnp.clip(jax.random.normal(field_key, shape, jnp.float32), -6.0, 6.0)
    scales = jnp.power(2.0, position) * rough
    return (values * scales).astype(jnp.bfloat16)


def draw_inputs(key, part):
    return scaled_field(key, 17)


def draw_cotangent(key, part):
    return scaled_field(key, 29)


def draw_kernel_taps(key, part):
    shape = (9, CHANNELS, CHANNELS)
    tap_key = jax.random.fold_in(key, 41)
    tap_scale = jnp.where(jnp.arange(9) == 4, 0.6, 0.3 / math.sqrt(8.0)) / math.sqrt(CHANNELS)
    values = jnp.clip(jax.random.normal(tap_key, shape, jnp.float32), -4.0, 4.0)
    return (values * tap_scale[:, None, None]).astype(jnp.float32)


def setup_inputs(seed: int = 0) -> dict:
    keys = jax.random.split(jax.random.key(seed), 4)
    return {
        "inputs": draw_inputs(jax.random.fold_in(keys[3], 71), 0),
        "cotangent": draw_cotangent(jax.random.fold_in(keys[3], 71), 0),
        "kernel_taps": draw_kernel_taps(jax.random.fold_in(keys[3], 71), 0),
    }


step_share = 0.06

def matmul(left_side, right_side):
    return jnp.dot(left_side, right_side, precision=lax.Precision.HIGHEST, preferred_element_type=jnp.float32)

def gradient_terms(inputs, cotangent):
    channels = inputs.shape[3]
    flat_cotangent = cotangent.reshape(-1, channels)
    collected = []
    for tap_index in range(9):
        row_off = tap_index // 3 - 1
        col_off = tap_index % 3 - 1
        shifted = jnp.roll(inputs, (-row_off, -col_off), axis=(1, 2))
        collected.append(lax.dot_general(shifted.reshape(-1, channels), flat_cotangent, (((0,), (0,)), ((), ())), preferred_element_type=jnp.float32))
    return jnp.stack(collected)

def phase_tables(freq_index, mapside, freq_count):
    row_shift = jnp.array([-1, -1, -1, 0, 0, 0, 1, 1, 1], dtype=jnp.int32)
    col_shift = jnp.array([-1, 0, 1, -1, 0, 1, -1, 0, 1], dtype=jnp.int32)
    half_width = mapside // 2 + 1
    first_freq = freq_index // half_width
    second_freq = freq_index % half_width
    turn_count = (first_freq[:, None] * row_shift[None, :] + second_freq[:, None] * col_shift[None, :]) % mapside
    phase_angle = turn_count.astype(jnp.float32) * (2.0 * math.pi / mapside)
    live_mask = (freq_index < freq_count).astype(jnp.float32)[:, None]
    return (jnp.cos(phase_angle) * live_mask, jnp.sin(phase_angle) * live_mask)

def inverse_tables(freq_index, mapside, freq_count):
    cos_table, sin_table = phase_tables(freq_index, mapside, freq_count)
    second_freq = freq_index % (mapside // 2 + 1)
    on_edge = (second_freq == 0) | (second_freq == mapside // 2)
    weight = jnp.where(on_edge, 1.0, 2.0).astype(jnp.float32) / (mapside * mapside)
    return (cos_table * weight[:, None], sin_table * weight[:, None])

def bjorck(real_part, imag_part):
    matrix_size = real_part.shape[0]
    identity = jnp.eye(matrix_size, dtype=jnp.float32)
    for iteration in range(2):
        products = matmul(real_part.T, jnp.concatenate([real_part, imag_part], axis=1))
        square = matmul(imag_part.T, imag_part)
        cross_part = products[:, matrix_size:]
        gram_real = products[:, :matrix_size] + square
        gram_imag = cross_part - cross_part.T
        mix_real = 1.5 * identity - 0.5 * gram_real
        mix_imag = -0.5 * gram_imag
        stacked = jnp.concatenate([jnp.concatenate([mix_real, mix_imag], axis=1), jnp.concatenate([-mix_imag, mix_real], axis=1)], axis=0)
        joined = matmul(jnp.concatenate([real_part, imag_part], axis=1), stacked)
        real_part, imag_part = (joined[:, :matrix_size], joined[:, matrix_size:])
    return (real_part, imag_part)

def reference(inputs, cotangent, kernel_taps):
    channels = CHANNELS
    input_blocks = inputs.reshape(N_DP * N_INNER, -1, MAPSIDE, MAPSIDE, channels)
    cotan_blocks = cotangent.reshape(N_DP * N_INNER, -1, MAPSIDE, MAPSIDE, channels)

    def accumulate(carried, matrices):
        return (carried + gradient_terms(matrices[0], matrices[1]), None)
    gradient, _ = lax.scan(accumulate, jnp.zeros((9, channels, channels), jnp.float32), (input_blocks, cotan_blocks))
    grad_norm = jnp.sqrt(jnp.sum(gradient * gradient))
    step_factor = step_share * math.sqrt(channels) / (grad_norm + 1e-06)
    updated = kernel_taps - step_factor * gradient
    flattened = updated.reshape(9, channels * channels)

    def per_freq(carried, freq_index):
        index_row = freq_index[None]
        cos_table, sin_table = phase_tables(index_row, MAPSIDE, FREQS)
        real_part = matmul(cos_table, flattened).reshape(channels, channels)
        imag_part = -matmul(sin_table, flattened).reshape(channels, channels)
        real_part, imag_part = bjorck(real_part, imag_part)
        weighted_cos, weighted_sin = inverse_tables(index_row, MAPSIDE, FREQS)
        contribution = matmul(weighted_cos.T, real_part.reshape(1, -1)) - matmul(weighted_sin.T, imag_part.reshape(1, -1))
        return (carried + contribution, None)
    rebuilt, _ = lax.scan(per_freq, jnp.zeros((9, channels * channels), jnp.float32), jnp.arange(FREQS, dtype=jnp.int32))
    return (math.sqrt(channels) * rebuilt).reshape(9, channels, channels)
```

```python
import functools
import math

import jax
import jax.numpy as jnp
from jax import lax
from jax.experimental import pallas as pl
from jax.experimental.pallas import tpu as pltpu
from jax.sharding import Mesh
from jax.sharding import PartitionSpec as P

AXES = ("dp_0", "dp_1", "dp_2", "inner_0", "inner_1")
INNER = ("inner_0", "inner_1")
DP = ("dp_0", "dp_1", "dp_2")
DP_INNER = DP + INNER
SIDE = 32
CHANNELS = 256
CELLS = SIDE * SIDE
STEP = 0.06 * math.sqrt(CHANNELS)
F32 = jnp.float32
BF16 = jnp.bfloat16
PLANE = 32
DEPTH = 16
CHUNKS = 3
MESH = pl.DeviceIdType.MESH
COS = [math.cos(2.0 * math.pi * k / SIDE) for k in range(SIDE)]
SIN = [math.sin(2.0 * math.pi * k / SIDE) for k in range(SIDE)]


def swap_groups(parts):
    lane = lax.broadcasted_iota(jnp.int32, parts[0].shape, 1)
    low = lane < 64
    even = (lane & 32) == 0
    v0, v1, v2, v3 = parts
    w0 = jnp.where(low, v0, pltpu.roll(v2, 64, 1))
    w2 = jnp.where(low, pltpu.roll(v0, 64, 1), v2)
    w1 = jnp.where(low, v1, pltpu.roll(v3, 64, 1))
    w3 = jnp.where(low, pltpu.roll(v1, 64, 1), v3)
    u0 = jnp.where(even, w0, pltpu.roll(w1, 32, 1))
    u1 = jnp.where(even, pltpu.roll(w0, 96, 1), w1)
    u2 = jnp.where(even, w2, pltpu.roll(w3, 32, 1))
    u3 = jnp.where(even, pltpu.roll(w2, 96, 1), w3)
    return u0, u1, u2, u3


def halves(value):
    high = value.astype(BF16)
    low = (value - high.astype(F32)).astype(BF16)
    return high, low


def product(left, right):
    dot = functools.partial(jnp.dot, preferred_element_type=F32)
    return dot(left[0], right[0]) + (dot(left[0], right[1]) + dot(left[1], right[0]))


def kernel(x_ref, ct_ref, taps_ref, out_ref, xt, cb, go, gr, s0, s1, r0, r1, t0, t1, u0, u1, zs, zr, gs, as_t, ar_t,
           as_g, ar_g, nv, nr, ks_t, kr_t, ks_g, kr_g, mat, ao, ar, fs, fr, pair_send, pair_recv, a_send, a_recv,
           b_send, b_recv, c_send, c_recv, one_send, one_recv):
    y = lax.axis_index("dp_0")
    zl = lax.axis_index("dp_1")
    c = lax.axis_index("dp_2")
    zh = lax.axis_index("inner_0")
    x = lax.axis_index("inner_1")
    z = zh * 8 + zl
    p = (y * 2 + c) * 4 + x

    def at_plane(q):
        return (q // 8, zl, (q // 4) % 2, zh, q % 4)

    def at_depth(w):
        return (y, w % 8, c, w // 8, x)

    def send(src, dst, send_sem, recv_sem, device):
        pltpu.make_async_remote_copy(
            src_ref=src, dst_ref=dst, send_sem=send_sem, recv_sem=recv_sem, device_id=device, device_id_type=MESH
        ).start()

    def drain(ref, sem):
        pltpu.make_async_copy(ref, ref, sem).wait()

    barrier = pltpu.get_barrier_semaphore()
    for d in range(1, PLANE):
        pl.semaphore_signal(barrier, inc=1, device_id=at_plane((p + d) % PLANE), device_id_type=MESH)
    for d in range(1, DEPTH):
        pl.semaphore_signal(barrier, inc=1, device_id=at_depth((z + d) % DEPTH), device_id_type=MESH)

    row = lax.broadcasted_iota(jnp.int32, (256, 256), 0)
    col = lax.broadcasted_iota(jnp.int32, (256, 256), 1)
    channel = (row & 192) + (row & 7) * 8 + ((row >> 5) & 1) * 4 + ((row >> 3) & 3)
    order = jnp.where(col == channel, 1.0, 0.0).astype(BF16)
    for k in range(4):
        xt[:, k * 256 : (k + 1) * 256] = lax.dot_general(
            order, x_ref[k * 256 : (k + 1) * 256, :], (((1,), (1,)), ((), ())), preferred_element_type=F32
        ).astype(BF16)
    for m in range(3):
        source = (row & 224) + ((row + (33 - m)) & 31)
        shift = jnp.where(col == source, 1.0, 0.0).astype(BF16)
        for k in range(4):
            rows = ct_ref[k * 256 : (k + 1) * 256, :]
            if m != 1:
                rows = jnp.dot(shift, rows, preferred_element_type=F32).astype(BF16)
            cb[m, 32 + k * 256 : 32 + (k + 1) * 256, :] = rows
        cb[m, 0:32, :] = cb[m, 1024:1056, :]
        cb[m, 1056:1088, :] = cb[m, 32:64, :]

    def depth_messages(block, dst):
        before, middle, after = [
            jnp.concatenate([block[3 * a + b : 3 * a + b + 1, :] for a in range(3)], axis=0) for b in range(3)
        ]
        both = after + before
        apart = after - before
        for w in range(DEPTH):
            if w == 0:
                upper, lower = middle + both, middle - both
            else:
                upper, lower = middle + COS[w] * both, -SIN[w] * apart
            dst[8 * w : 8 * w + 3, :] = upper
            dst[8 * w + 3 : 8 * w + 6, :] = lower
        return None

    def depth_send(src, dst, sem):
        for d in range(1, DEPTH):
            w = (z + d) % DEPTH
            send(src.at[pl.ds(pl.multiple_of(w * 8, 8), 8)], dst.at[pl.ds(pl.multiple_of(z * 8, 8), 8)],
                 one_send.at[sem], one_recv.at[sem], at_depth(w))
        own = pl.ds(pl.multiple_of(z * 8, 8), 8)
        dst[own, :] = src[own, :]

    def depth_wait(dst, sem):
        drain(dst.at[pl.ds(0, 120)], one_recv.at[sem])

    def plane_messages(src, dst):
        parts = [src[pl.ds(m, DEPTH, stride=8), :] for m in range(6)]

        @pl.when(z != 0)
        def _():
            real_sum, real_gap = parts[2] + parts[0], parts[2] - parts[0]
            imag_sum, imag_gap = parts[5] + parts[3], parts[5] - parts[3]
            for k in range(17):
                upper, upper_gap = parts[1] + COS[k] * real_sum, SIN[k] * imag_gap
                lower, lower_gap = parts[4] + COS[k] * imag_sum, SIN[k] * real_gap
                dst[k, 0:16, :] = upper + upper_gap
                dst[k, 16:32, :] = lower - lower_gap
                if 0 < k < 16:
                    dst[32 - k, 0:16, :] = upper - upper_gap
                    dst[32 - k, 16:32, :] = lower + lower_gap

        @pl.when(z == 0)
        def _():
            for half in range(2):
                first, mid, last = parts[3 * half : 3 * half + 3]
                total, gap = last + first, last - first
                dst[16 * half, 0:16, :] = mid + total
                dst[16 * half, 16:32, :] = mid - total
                for k in range(1, 16):
                    dst[16 * half + k, 0:16, :] = mid + COS[k] * total
                    dst[16 * half + k, 16:32, :] = -SIN[k] * gap

    def plane_send(src, dst, sem):
        for d in range(1, PLANE):
            q = (p + d) % PLANE
            send(src.at[q], dst.at[p], one_send.at[sem], one_recv.at[sem], at_plane(q))
        dst[p] = src[p]

    def plane_wait(dst, sem):
        drain(dst.at[pl.ds(0, PLANE - 1)], one_recv.at[sem])

    as_t[...] = jnp.zeros_like(as_t)
    as_g[...] = jnp.zeros_like(as_g)
    fs[...] = jnp.zeros_like(fs)
    depth_messages(taps_ref[...], as_t)

    def chunk_out(ch):
        for t in range(3):
            drain(gr.at[3 * ch + t], pair_recv.at[3 * ch + t])
        for t in range(3):
            for yy in range(4):
                for xx in range(4):
                    s0[ch, xx, t, yy] = go[c, 3 * ch + t, yy, xx, 0] + gr[3 * ch + t, yy, xx, 0]
                    s1[ch, yy, t, xx] = go[c, 3 * ch + t, yy, xx, 1] + gr[3 * ch + t, yy, xx, 1]
        for d in (1, 3, 2):
            xx, yy = (x + d) % 4, (y + d) % 4
            send(s0.at[ch, xx], r0.at[ch, d - 1], a_send.at[0], a_recv.at[ch], (y, zl, c, zh, xx))
            send(s1.at[ch, yy], r1.at[ch, d - 1], a_send.at[1], a_recv.at[3 + ch], (yy, zl, c, zh, x))

    def chunk_on(ch):
        drain(r0.at[ch], a_recv.at[ch])
        for t in range(3):
            for yy in range(4):
                t0[ch, yy, t] = (s0[ch, x, t, yy] + r0[ch, 0, t, yy]) + (r0[ch, 1, t, yy] + r0[ch, 2, t, yy])
        for d in (1, 3, 2):
            yy = (y + d) % 4
            send(t0.at[ch, yy], u0.at[ch, d - 1], b_send.at[0], b_recv.at[ch], (yy, zl, c, zh, x))
        drain(r1.at[ch], a_recv.at[3 + ch])
        for t in range(3):
            for xx in range(4):
                t1[ch, xx, t] = (s1[ch, y, t, xx] + r1[ch, 0, t, xx]) + (r1[ch, 1, t, xx] + r1[ch, 2, t, xx])
        for d in (1, 3, 2):
            xx = (x + d) % 4
            send(t1.at[ch, xx], u1.at[ch, d - 1], b_send.at[1], b_recv.at[3 + ch], (y, zl, c, zh, xx))

    def chunk_in(ch):
        drain(u0.at[ch], b_recv.at[ch])
        drain(u1.at[ch], b_recv.at[3 + ch])
        for t in range(3):
            first = (t0[ch, y, t] + u0[ch, 0, t]) + (u0[ch, 1, t] + u0[ch, 2, t])
            second = (t1[ch, x, t] + u1[ch, 0, t]) + (u1[ch, 1, t] + u1[ch, 2, t])
            for w in range(8):
                zs[w, 3 * ch + t : 3 * ch + t + 1, :] = first[w : w + 1, :]
                zs[8 + w, 3 * ch + t : 3 * ch + t + 1, :] = second[w : w + 1, :]

    for t in range(9):
        a, b = t // 3 - 1, t % 3
        grad = jnp.dot(xt[...], cb[b, 32 - 32 * a : 32 - 32 * a + CELLS, :], preferred_element_type=F32)
        for yc in range(8):
            for h in range(2):
                parts = [grad[yc * 32 + i * 8 : yc * 32 + i * 8 + 8, h * 128 : h * 128 + 128] for i in range(4)]
                for xx, part in enumerate(swap_groups(parts)):
                    go[yc % 2, t, yc // 2, xx, h] = part
        if t == 0:
            pl.semaphore_wait(barrier, PLANE + DEPTH - 2)
            depth_send(as_t, ar_t, 0)
        send(go.at[1 - c, t], gr.at[t], pair_send, pair_recv.at[t], (y, zl, 1 - c, zh, x))
        if t == 4:
            chunk_out(0)
        if t == 7:
            chunk_out(1)
    chunk_out(2)
    for ch in range(CHUNKS):
        chunk_on(ch)
    depth_wait(ar_t, 0)
    plane_messages(ar_t, ks_t)
    plane_send(ks_t, kr_t, 2)
    for ch in range(CHUNKS):
        chunk_in(ch)

    for d in range(1, DEPTH):
        w = (z + d) % DEPTH
        send(zs.at[w], zr.at[d - 1], c_send, c_recv, at_depth(w))
    drain(zr, c_recv)
    block = zs[z]
    for d in range(DEPTH - 1):
        block = block + zr[d]
    gs[...] = block
    depth_messages(gs[...], as_g)
    squares = jnp.sum(block * block, axis=0, keepdims=True)
    for w in range(DEPTH):
        as_g[8 * w + 6 : 8 * w + 7, :] = squares
    depth_send(as_g, ar_g, 1)
    depth_wait(ar_g, 1)

    nv[...] = jnp.sum(ar_g[pl.ds(6, DEPTH, stride=8), :], axis=0, keepdims=True)
    for d in range(1, PLANE):
        q = (p + d) % PLANE
        send(nv, nr.at[d - 1], one_send.at[6], one_recv.at[6], at_plane(q))
    plane_messages(ar_g, ks_g)
    plane_send(ks_g, kr_g, 3)
    plane_wait(kr_t, 2)
    drain(nr, one_recv.at[6])
    total = nv[...]
    for d in range(PLANE - 1):
        total = total + nr[d]
    norm = jnp.sqrt(jnp.sum(total, axis=1, keepdims=True))
    factor = jnp.broadcast_to(STEP / (norm + 1e-6), (8, 128))
    plane_wait(kr_g, 3)

    for yc in range(8):
        for m in range(2):
            for h in range(2):
                rows = slice(m * 16 + h * 8, m * 16 + h * 8 + 8)
                parts = [kr_t[yc * 4 + xx, rows, :] - factor * kr_g[yc * 4 + xx, rows, :] for xx in range(4)]
                for i, part in enumerate(swap_groups(parts)):
                    mat[m, yc * 32 + i * 8 : yc * 32 + i * 8 + 8, h * 128 : h * 128 + 128] = part

    joint = jnp.where((z == 0) & (p % 16 == 0), 0.0, 1.0).astype(F32)
    for _ in range(2):
        real, imag = mat[0], mat[1]
        real_2, imag_2 = halves(real), halves(imag)
        real_t, imag_t = halves(real.T), halves(imag.T)
        first = product(real_t, real_2)
        second = product(imag_t, imag_2)
        cross = product(real_t, imag_2) - product(imag_t, real_2)
        eye = jnp.where(row == col, 1.5, 0.0)
        mix_first = halves(eye - 0.5 * (first + joint * second))
        mix_second = halves(eye - 0.5 * (second + joint * first))
        mix_cross = halves((-0.5 * joint) * cross)
        mat[0] = product(real_2, mix_first) - product(imag_2, mix_cross)
        mat[1] = product(real_2, mix_cross) + product(imag_2, mix_second)

    for yc in range(8):
        for m in range(2):
            for h in range(2):
                parts = [mat[m, yc * 32 + i * 8 : yc * 32 + i * 8 + 8, h * 128 : h * 128 + 128] for i in range(4)]
                for xx, part in enumerate(swap_groups(parts)):
                    ao[yc * 4 + xx, m * 16 + h * 8 : m * 16 + h * 8 + 8, :] = part
    plane_send(ao, ar, 4)
    plane_wait(ar, 4)

    def summed(first, last, base):
        zero = jnp.zeros((DEPTH, 128), F32)
        real_0 = imag_0 = real_c = real_s = imag_c = imag_s = zero
        for k in range(first, last):
            real, imag = ar[k, 0:16, :], ar[k, 16:32, :]
            ck, sk = COS[k - base], SIN[k - base]
            real_0, imag_0 = real_0 + real, imag_0 + imag
            real_c, real_s = real_c + ck * real, real_s + sk * real
            imag_c, imag_s = imag_c + ck * imag, imag_s + sk * imag
        return real_0, imag_0, real_c, real_s, imag_c, imag_s

    @pl.when(z != 0)
    def _():
        real_0, imag_0, real_c, real_s, imag_c, imag_s = summed(0, 32, 0)
        parts = (real_c + imag_s, real_0, real_c - imag_s, imag_c - real_s, imag_0, imag_c + real_s)
        for m, part in enumerate(parts):
            fs[pl.ds(m, DEPTH, stride=8), :] = 2.0 * part

    @pl.when(z == 0)
    def _():
        for half in range(2):
            real_0, imag_0, real_c, real_s, imag_c, imag_s = summed(16 * half + 1, 16 * half + 16, 16 * half)
            one, other = ar[16 * half, 0:16, :], ar[16 * half, 16:32, :]
            parts = (
                2.0 * (real_c + imag_s) + (one - other),
                2.0 * real_0 + (one + other),
                2.0 * (real_c - imag_s) + (one - other),
            )
            for m, part in enumerate(parts):
                fs[pl.ds(3 * half + m, DEPTH, stride=8), :] = part

    depth_send(fs, fr, 5)
    depth_wait(fr, 5)
    plain = fr[8:16, :]
    cosine = COS[1] * fr[8:16, :]
    sine = SIN[1] * fr[8:16, :]
    for w in range(2, DEPTH):
        tile = fr[8 * w : 8 * w + 8, :]
        plain, cosine, sine = plain + tile, cosine + COS[w] * tile, sine + SIN[w] * tile
    edge = fr[0:8, :]
    for a in range(3):
        first, last = edge[a : a + 1, :], edge[a + 3 : a + 4, :]
        even, odd = first + last, first - last
        out_ref[3 * a + 1 : 3 * a + 2, :] = (plain[a : a + 1, :] + even) * (1.0 / 64.0)
        out_ref[3 * a : 3 * a + 1, :] = (cosine[a : a + 1, :] + sine[a + 3 : a + 4, :] + odd) * (1.0 / 64.0)
        out_ref[3 * a + 2 : 3 * a + 3, :] = (cosine[a : a + 1, :] - sine[a + 3 : a + 4, :] + odd) * (1.0 / 64.0)

    drain(go.at[0], pair_send)
    drain(r0, a_send.at[0])
    drain(r1, a_send.at[1])
    drain(u0, b_send.at[0])
    drain(u1, b_send.at[1])
    drain(zr, c_send)
    for n, ref in ((0, as_t), (1, as_g), (5, fs)):
        drain(ref.at[pl.ds(0, 120)], one_send.at[n])
    for n, ref in ((2, ks_t), (3, ks_g), (4, ao)):
        drain(ref.at[pl.ds(0, PLANE - 1)], one_send.at[n])
    drain(nr, one_send.at[6])


def body(inputs, cotangent, kernel_taps):
    vmem = lambda *shape: pltpu.VMEM(shape, F32)
    out = pl.pallas_call(
        kernel,
        out_shape=jax.ShapeDtypeStruct((9, 128), F32),
        in_specs=[pl.BlockSpec(memory_space=pltpu.VMEM)] * 3,
        out_specs=pl.BlockSpec(memory_space=pltpu.VMEM),
        scratch_shapes=[
            pltpu.VMEM((CHANNELS, CELLS), BF16),
            pltpu.VMEM((3, CELLS + 64, CHANNELS), BF16),
            vmem(2, 9, 4, 4, 2, 8, 128),
            vmem(9, 4, 4, 2, 8, 128),
            vmem(3, 4, 3, 4, 8, 128),
            vmem(3, 4, 3, 4, 8, 128),
            vmem(3, 3, 3, 4, 8, 128),
            vmem(3, 3, 3, 4, 8, 128),
            vmem(3, 4, 3, 8, 128),
            vmem(3, 4, 3, 8, 128),
            vmem(3, 3, 3, 8, 128),
            vmem(3, 3, 3, 8, 128),
            vmem(DEPTH, 9, 128),
            vmem(DEPTH - 1, 9, 128),
            vmem(9, 128),
            vmem(128, 128),
            vmem(128, 128),
            vmem(128, 128),
            vmem(128, 128),
            vmem(1, 128),
            vmem(PLANE - 1, 1, 128),
            vmem(PLANE, 32, 128),
            vmem(PLANE, 32, 128),
            vmem(PLANE, 32, 128),
            vmem(PLANE, 32, 128),
            vmem(2, 256, 256),
            vmem(PLANE, 32, 128),
            vmem(PLANE, 32, 128),
            vmem(128, 128),
            vmem(128, 128),
            pltpu.SemaphoreType.DMA,
            pltpu.SemaphoreType.DMA((9,)),
            pltpu.SemaphoreType.DMA((2,)),
            pltpu.SemaphoreType.DMA((6,)),
            pltpu.SemaphoreType.DMA((2,)),
            pltpu.SemaphoreType.DMA((6,)),
            pltpu.SemaphoreType.DMA,
            pltpu.SemaphoreType.DMA,
            pltpu.SemaphoreType.DMA((7,)),
            pltpu.SemaphoreType.DMA((7,)),
        ],
        compiler_params=pltpu.CompilerParams(collective_id=0, has_side_effects=True, vmem_limit_bytes=50 * 2**20),
        name="step",
    )(inputs.reshape(CELLS, CHANNELS), cotangent.reshape(CELLS, CHANNELS), kernel_taps.reshape(9, 128))
    return out.reshape(9, 4, 32)


def solution(mesh):
    torus = Mesh(mesh.devices.reshape(4, 8, 2, 2, 4), AXES)
    return jax.shard_map(
        body,
        mesh=torus,
        in_specs=(P(DP_INNER, None, None, None), P(DP_INNER, None, None, None), P(None, DP, INNER)),
        out_specs=P(None, DP, INNER),
        check_vma=False,
    )
```

```python
import functools
import math

import jax
import jax.numpy as jnp
from jax import lax
from jax.experimental import pallas as pl
from jax.experimental.pallas import tpu as pltpu
from jax.sharding import Mesh
from jax.sharding import PartitionSpec as P

AXES = ("dp_0", "dp_1", "dp_2", "inner_0", "inner_1")
INNER = ("inner_0", "inner_1")
DP = ("dp_0", "dp_1", "dp_2")
DP_INNER = DP + INNER
SIDE = 32
CHANNELS = 256
CELLS = SIDE * SIDE
STEP = 0.06 * math.sqrt(CHANNELS)
F32 = jnp.float32
BF16 = jnp.bfloat16
PLANE = 32
DEPTH = 16
CHUNKS = 3
MESH = pl.DeviceIdType.MESH
PEERS = sorted(
    [(dy, dc, dx) for dy in range(4) for dc in range(2) for dx in range(4) if dy or dc or dx],
    key=lambda m: -(min(m[0], 4 - m[0]) + min(m[2], 4 - m[2])),
)
STEPS = sorted(range(1, DEPTH), key=lambda d: -min(d, DEPTH - d))
COS = [math.cos(2.0 * math.pi * k / SIDE) for k in range(SIDE)]
SIN = [math.sin(2.0 * math.pi * k / SIDE) for k in range(SIDE)]


def swap_groups(parts):
    lane = lax.broadcasted_iota(jnp.int32, parts[0].shape, 1)
    low = lane < 64
    even = (lane & 32) == 0
    v0, v1, v2, v3 = parts
    w0 = jnp.where(low, v0, pltpu.roll(v2, 64, 1))
    w2 = jnp.where(low, pltpu.roll(v0, 64, 1), v2)
    w1 = jnp.where(low, v1, pltpu.roll(v3, 64, 1))
    w3 = jnp.where(low, pltpu.roll(v1, 64, 1), v3)
    u0 = jnp.where(even, w0, pltpu.roll(w1, 32, 1))
    u1 = jnp.where(even, pltpu.roll(w0, 96, 1), w1)
    u2 = jnp.where(even, w2, pltpu.roll(w3, 32, 1))
    u3 = jnp.where(even, pltpu.roll(w2, 96, 1), w3)
    return u0, u1, u2, u3


def halves(value):
    high = value.astype(BF16)
    low = (value - high.astype(F32)).astype(BF16)
    return high, low


def product(left, right):
    dot = functools.partial(jnp.dot, preferred_element_type=F32)
    return dot(left[0], right[0]) + (dot(left[0], right[1]) + dot(left[1], right[0]))


def kernel(x_hbm, ct_hbm, taps_hbm, out_ref, x_ref, ct_ref, taps_ref, xt, cb, go, gr, s0, s1, r0, r1, t0, t1, u0, u1, zs, zr, gs, as_t, ar_t,
           as_g, ar_g, nv, nr, ks_t, kr_t, ks_g, kr_g, mat, ao, ar, fs, fr, pair_send, pair_recv, a_send, a_recv,
           b_send, b_recv, c_send, c_recv, one_send, one_recv, load_sem):
    y = lax.axis_index("dp_0")
    zl = lax.axis_index("dp_1")
    c = lax.axis_index("dp_2")
    zh = lax.axis_index("inner_0")
    x = lax.axis_index("inner_1")
    z = zh * 8 + zl
    p = (y * 2 + c) * 4 + x

    ys = [y] + [lax.rem(y + d, 4) for d in range(1, 4)]
    xs = [x] + [lax.rem(x + d, 4) for d in range(1, 4)]
    cores = [c, 1 - c]
    depths = [z] + [lax.rem(z + d, DEPTH) for d in range(1, DEPTH)]

    def at_plane(peer):
        dy, dc, dx = peer
        return (ys[dy], zl, cores[dc], zh, xs[dx])

    def place(peer):
        dy, dc, dx = peer
        return (ys[dy] * 2 + cores[dc]) * 4 + xs[dx]

    def at_depth(d):
        return (y, lax.rem(depths[d], 8), c, lax.div(depths[d], 8), x)

    def send(src, dst, send_sem, recv_sem, device):
        pltpu.make_async_remote_copy(
            src_ref=src, dst_ref=dst, send_sem=send_sem, recv_sem=recv_sem, device_id=device, device_id_type=MESH
        ).start()

    def drain(ref, sem):
        pltpu.make_async_copy(ref, ref, sem).wait()

    pending = []

    def finish():
        for ref, sem in pending:
            drain(ref, sem)

    loads = [
        pltpu.make_async_copy(src, dst, load_sem.at[n])
        for n, (src, dst) in enumerate(((x_hbm, x_ref), (ct_hbm, ct_ref), (taps_hbm, taps_ref)))
    ]
    for load in loads:
        load.start()
    barrier = pltpu.get_barrier_semaphore()
    for d in STEPS:
        pl.semaphore_signal(barrier, inc=1, device_id=at_depth(d), device_id_type=MESH)
    for peer in PEERS:
        pl.semaphore_signal(barrier, inc=1, device_id=at_plane(peer), device_id_type=MESH)

    row = lax.broadcasted_iota(jnp.int32, (256, 256), 0)
    col = lax.broadcasted_iota(jnp.int32, (256, 256), 1)
    channel = (row & 192) + (row & 7) * 8 + ((row >> 5) & 1) * 4 + ((row >> 3) & 3)
    order = jnp.where(col == channel, 1.0, 0.0).astype(BF16)
    loads[0].wait()
    for k in range(4):
        xt[:, k * 256 : (k + 1) * 256] = lax.dot_general(
            order, x_ref[k * 256 : (k + 1) * 256, :], (((1,), (1,)), ((), ())), preferred_element_type=F32
        ).astype(BF16)
    loads[1].wait()
    for m in range(3):
        source = (row & 224) + ((row + (33 - m)) & 31)
        shift = jnp.where(col == source, 1.0, 0.0).astype(BF16)
        for k in range(4):
            rows = ct_ref[k * 256 : (k + 1) * 256, :]
            if m != 1:
                rows = jnp.dot(shift, rows, preferred_element_type=F32).astype(BF16)
            cb[m, 32 + k * 256 : 32 + (k + 1) * 256, :] = rows
        cb[m, 0:32, :] = cb[m, 1024:1056, :]
        cb[m, 1056:1088, :] = cb[m, 32:64, :]

    def depth_messages(block, dst):
        before, middle, after = [
            jnp.concatenate([block[3 * a + b : 3 * a + b + 1, :] for a in range(3)], axis=0) for b in range(3)
        ]
        both = after + before
        apart = after - before
        for w in range(DEPTH):
            if w == 0:
                upper, lower = middle + both, middle - both
            else:
                upper, lower = middle + COS[w] * both, -SIN[w] * apart
            dst[8 * w : 8 * w + 3, :] = upper
            dst[8 * w + 3 : 8 * w + 6, :] = lower
        return None

    def depth_send(src, dst, sem):
        for d in STEPS:
            slot = (4 - d) % DEPTH
            send(src.at[pl.ds(pl.multiple_of(depths[d] * 8, 8), 8)], dst.at[pl.ds(8 * slot, 8)],
                 one_send.at[sem], one_recv.at[sem + slot // 8], at_depth(d))
        dst[32:40, :] = src[pl.ds(pl.multiple_of(z * 8, 8), 8), :]
        pending.append((src.at[pl.ds(0, 120)], one_send.at[sem]))

    def depth_wait(dst, sem, half):
        drain(dst.at[pl.ds(0, 64 if half else 56)], one_recv.at[sem + half])

    def plane_messages(src, dst, half):
        parts = [src[pl.ds(64 * half + m, 8, stride=8), :] for m in range(6)]

        @pl.when(z != 0)
        def _():
            real_sum, real_gap = parts[2] + parts[0], parts[2] - parts[0]
            imag_sum, imag_gap = parts[5] + parts[3], parts[5] - parts[3]
            for k in range(17):
                upper, upper_gap = parts[1] + COS[k] * real_sum, SIN[k] * imag_gap
                lower, lower_gap = parts[4] + COS[k] * imag_sum, SIN[k] * real_gap
                dst[half, k, 0] = upper + upper_gap
                dst[half, k, 1] = lower - lower_gap
                if 0 < k < 16:
                    dst[half, 32 - k, 0] = upper - upper_gap
                    dst[half, 32 - k, 1] = lower + lower_gap

        @pl.when(z == 0)
        def _():
            for edge in range(2):
                first, mid, last = parts[3 * edge : 3 * edge + 3]
                total, gap = last + first, last - first
                dst[half, 16 * edge, 0] = mid + total
                dst[half, 16 * edge, 1] = mid - total
                for k in range(1, 16):
                    dst[half, 16 * edge + k, 0] = mid + COS[k] * total
                    dst[half, 16 * edge + k, 1] = -SIN[k] * gap

    def plane_send(src, dst, half, sem):
        for peer in PEERS:
            send(src.at[half, place(peer)], dst.at[half, p], one_send.at[sem + half], one_recv.at[sem + half], at_plane(peer))
        dst[half, p] = src[half, p]
        pending.append((src.at[half, pl.ds(0, PLANE - 1)], one_send.at[sem + half]))

    def plane_wait(dst, half, sem):
        drain(dst.at[half, pl.ds(0, PLANE - 1)], one_recv.at[sem + half])

    sublane = lax.broadcasted_iota(jnp.int32, (8, 128), 0)

    def turned(low, high, shift):
        rest = lax.rem(shift, 8)
        kept = (sublane >= rest) == (shift < 8)
        low, high = pltpu.roll(low, rest, 0), pltpu.roll(high, rest, 0)
        return jnp.where(kept, low, high), jnp.where(kept, high, low)

    as_t[...] = jnp.zeros_like(as_t)
    as_g[...] = jnp.zeros_like(as_g)
    fs[...] = jnp.zeros_like(fs)
    loads[2].wait()
    depth_messages(jnp.concatenate([taps_ref[:, i, :] for i in range(4)], axis=1), as_t)

    def chunk_out(ch):
        for t in range(3):
            drain(gr.at[3 * ch + t], pair_recv.at[3 * ch + t])
        for t in range(3):
            for yy in range(4):
                for xx in range(4):
                    s0[ch, xx, t, yy] = go[c, 3 * ch + t, yy, xx, 0] + gr[3 * ch + t, yy, xx, 0]
                    s1[ch, yy, t, xx] = go[c, 3 * ch + t, yy, xx, 1] + gr[3 * ch + t, yy, xx, 1]
        for d in (1, 3, 2):
            xx, yy = xs[d], ys[d]
            send(s0.at[ch, xx], r0.at[ch, d - 1], a_send.at[0], a_recv.at[ch], (y, zl, c, zh, xx))
            send(s1.at[ch, yy], r1.at[ch, d - 1], a_send.at[1], a_recv.at[3 + ch], (yy, zl, c, zh, x))

    def chunk_on(ch):
        drain(r0.at[ch], a_recv.at[ch])
        for t in range(3):
            for yy in range(4):
                t0[ch, yy, t] = (s0[ch, x, t, yy] + r0[ch, 0, t, yy]) + (r0[ch, 1, t, yy] + r0[ch, 2, t, yy])
        for d in (1, 3, 2):
            yy = ys[d]
            send(t0.at[ch, yy], u0.at[ch, d - 1], b_send.at[0], b_recv.at[ch], (yy, zl, c, zh, x))
        drain(r1.at[ch], a_recv.at[3 + ch])
        for t in range(3):
            for xx in range(4):
                t1[ch, xx, t] = (s1[ch, y, t, xx] + r1[ch, 0, t, xx]) + (r1[ch, 1, t, xx] + r1[ch, 2, t, xx])
        for d in (1, 3, 2):
            xx = xs[d]
            send(t1.at[ch, xx], u1.at[ch, d - 1], b_send.at[1], b_recv.at[3 + ch], (y, zl, c, zh, xx))

    def chunk_in(ch):
        drain(u0.at[ch], b_recv.at[ch])
        drain(u1.at[ch], b_recv.at[3 + ch])
        for t in range(3):
            first = (t0[ch, y, t] + u0[ch, 0, t]) + (u0[ch, 1, t] + u0[ch, 2, t])
            second = (t1[ch, x, t] + u1[ch, 0, t]) + (u1[ch, 1, t] + u1[ch, 2, t])
            for w in range(8):
                zs[w, 3 * ch + t : 3 * ch + t + 1, :] = first[w : w + 1, :]
                zs[8 + w, 3 * ch + t : 3 * ch + t + 1, :] = second[w : w + 1, :]

    for t in range(9):
        a, b = t // 3 - 1, t % 3
        grad = jnp.dot(xt[...], cb[b, 32 - 32 * a : 32 - 32 * a + CELLS, :], preferred_element_type=F32)
        for yc in range(8):
            for h in range(2):
                parts = [grad[yc * 32 + i * 8 : yc * 32 + i * 8 + 8, h * 128 : h * 128 + 128] for i in range(4)]
                for xx, part in enumerate(swap_groups(parts)):
                    go[yc % 2, t, yc // 2, xx, h] = part
        if t == 0:
            pl.semaphore_wait(barrier, PLANE + DEPTH - 2)
            depth_send(as_t, ar_t, 0)
        send(go.at[1 - c, t], gr.at[t], pair_send, pair_recv.at[t], (y, zl, 1 - c, zh, x))
        if t == 4:
            chunk_out(0)
        if t == 7:
            chunk_out(1)
    chunk_out(2)
    pending.append((go.at[0], pair_send))
    pending.append((r0, a_send.at[0]))
    pending.append((r1, a_send.at[1]))
    for ch in range(CHUNKS):
        chunk_on(ch)
    pending.append((u0, b_send.at[0]))
    pending.append((u1, b_send.at[1]))
    for half in range(2):
        depth_wait(ar_t, 0, half)
        plane_messages(ar_t, ks_t, half)
        plane_send(ks_t, kr_t, half, 4)
    for ch in range(CHUNKS):
        chunk_in(ch)
    for d in STEPS:
        send(zs.at[depths[d]], zr.at[d - 1], c_send, c_recv, at_depth(d))
    drain(zr, c_recv)
    pending.append((zr, c_send))
    block = zs[z]
    for d in range(DEPTH - 1):
        block = block + zr[d]
    gs[...] = block
    depth_messages(gs[...], as_g)
    squares = jnp.sum(block * block, axis=0, keepdims=True)
    for w in range(DEPTH):
        as_g[8 * w + 6 : 8 * w + 7, :] = squares
    depth_send(as_g, ar_g, 2)
    depth_wait(ar_g, 2, 0)
    plane_messages(ar_g, ks_g, 0)
    plane_send(ks_g, kr_g, 0, 6)
    depth_wait(ar_g, 2, 1)
    plane_messages(ar_g, ks_g, 1)
    plane_send(ks_g, kr_g, 1, 6)
    nv[...] = jnp.sum(ar_g[pl.ds(6, DEPTH, stride=8), :], axis=0, keepdims=True)
    for d, peer in enumerate(PEERS):
        send(nv, nr.at[d], one_send.at[12], one_recv.at[12], at_plane(peer))
    pending.append((nr, one_send.at[12]))
    for half in range(2):
        plane_wait(kr_t, half, 4)
    drain(nr, one_recv.at[12])
    total = nv[...]
    for d in range(PLANE - 1):
        total = total + nr[d]
    norm = jnp.sqrt(jnp.sum(total, axis=1, keepdims=True))
    factor = jnp.broadcast_to(STEP / (norm + 1e-6), (8, 128))
    for half in range(2):
        plane_wait(kr_g, half, 6)

    onward = depths[12]
    for yc in range(8):
        for m in range(2):
            parts = []
            for xx in range(4):
                near, far = [kr_t[n, yc * 4 + xx, m] - factor * kr_g[n, yc * 4 + xx, m] for n in range(2)]
                parts.append(turned(near, far, onward))
            for h in range(2):
                for i, part in enumerate(swap_groups([pair[h] for pair in parts])):
                    mat[m, yc * 32 + i * 8 : yc * 32 + i * 8 + 8, h * 128 : h * 128 + 128] = part

    joint = jnp.where((z == 0) & (p % 16 == 0), 0.0, 1.0).astype(F32)
    for _ in range(2):
        real, imag = mat[0], mat[1]
        real_2, imag_2 = halves(real), halves(imag)
        real_t, imag_t = halves(real.T), halves(imag.T)
        first = product(real_t, real_2)
        second = product(imag_t, imag_2)
        cross = product(real_t, imag_2) - product(imag_t, real_2)
        eye = jnp.where(row == col, 1.5, 0.0)
        mix_first = halves(eye - 0.5 * (first + joint * second))
        mix_second = halves(eye - 0.5 * (second + joint * first))
        mix_cross = halves((-0.5 * joint) * cross)
        mat[0] = product(real_2, mix_first) - product(imag_2, mix_cross)
        mat[1] = product(real_2, mix_cross) + product(imag_2, mix_second)

    back = lax.rem(20 - z, DEPTH)
    for yc in range(8):
        for m in range(2):
            low, high = [
                swap_groups(
                    [mat[m, yc * 32 + i * 8 : yc * 32 + i * 8 + 8, h * 128 : h * 128 + 128] for i in range(4)]
                )
                for h in range(2)
            ]
            for xx in range(4):
                ao[0, yc * 4 + xx, m], ao[1, yc * 4 + xx, m] = turned(low[xx], high[xx], back)
    plane_send(ao, ar, 1, 8)
    plane_send(ao, ar, 0, 8)

    def summed(half, first, last, base):
        real_0 = imag_0 = real_c = real_s = imag_c = imag_s = jnp.zeros((8, 128), F32)
        for k in range(first, last):
            real, imag = ar[half, k, 0], ar[half, k, 1]
            ck, sk = COS[k - base], SIN[k - base]
            real_0, imag_0 = real_0 + real, imag_0 + imag
            real_c, real_s = real_c + ck * real, real_s + sk * real
            imag_c, imag_s = imag_c + ck * imag, imag_s + sk * imag
        return real_0, imag_0, real_c, real_s, imag_c, imag_s

    for half in (1, 0):
        plane_wait(ar, half, 8)

        @pl.when(z != 0)
        def _():
            real_0, imag_0, real_c, real_s, imag_c, imag_s = summed(half, 0, 32, 0)
            parts = (real_c + imag_s, real_0, real_c - imag_s, imag_c - real_s, imag_0, imag_c + real_s)
            for m, part in enumerate(parts):
                fs[pl.ds(64 * half + m, 8, stride=8), :] = 2.0 * part

        @pl.when(z == 0)
        def _():
            for edge in range(2):
                base = 16 * edge
                real_0, imag_0, real_c, real_s, imag_c, imag_s = summed(half, base + 1, base + 16, base)
                one, other = ar[half, base, 0], ar[half, base, 1]
                parts = (
                    2.0 * (real_c + imag_s) + (one - other),
                    2.0 * real_0 + (one + other),
                    2.0 * (real_c - imag_s) + (one - other),
                )
                for m, part in enumerate(parts):
                    fs[pl.ds(64 * half + 3 * edge + m, 8, stride=8), :] = part

        own = pl.ds(pl.multiple_of(z * 8, 8), 8)
        for d in STEPS:
            slot = (d + 4) % DEPTH
            if slot // 8 == half:
                send(fs.at[pl.ds(8 * slot, 8)], fr.at[own], one_send.at[10], one_recv.at[10], at_depth(d))
        if half == 0:
            fr[own, :] = fs[32:40, :]
    pending.append((fs.at[pl.ds(0, 120)], one_send.at[10]))
    drain(fr.at[pl.ds(0, 120)], one_recv.at[10])
    plain = fr[8:16, :]
    cosine = COS[1] * fr[8:16, :]
    sine = SIN[1] * fr[8:16, :]
    for w in range(2, DEPTH):
        tile = fr[8 * w : 8 * w + 8, :]
        plain, cosine, sine = plain + tile, cosine + COS[w] * tile, sine + SIN[w] * tile
    edge = fr[0:8, :]
    for a in range(3):
        first, last = edge[a : a + 1, :], edge[a + 3 : a + 4, :]
        even, odd = first + last, first - last
        out_ref[3 * a + 1 : 3 * a + 2, :] = (plain[a : a + 1, :] + even) * (1.0 / 64.0)
        out_ref[3 * a : 3 * a + 1, :] = (cosine[a : a + 1, :] + sine[a + 3 : a + 4, :] + odd) * (1.0 / 64.0)
        out_ref[3 * a + 2 : 3 * a + 3, :] = (cosine[a : a + 1, :] - sine[a + 3 : a + 4, :] + odd) * (1.0 / 64.0)

    finish()


def body(inputs, cotangent, kernel_taps):
    vmem = lambda *shape: pltpu.VMEM(shape, F32)
    out = pl.pallas_call(
        kernel,
        out_shape=jax.ShapeDtypeStruct((9, 128), F32),
        in_specs=[pl.BlockSpec(memory_space=pl.ANY)] * 3,
        out_specs=pl.BlockSpec(memory_space=pltpu.VMEM),
        scratch_shapes=[
            pltpu.VMEM((CELLS, CHANNELS), BF16),
            pltpu.VMEM((CELLS, CHANNELS), BF16),
            vmem(9, 4, 32),
            pltpu.VMEM((CHANNELS, CELLS), BF16),
            pltpu.VMEM((3, CELLS + 64, CHANNELS), BF16),
            vmem(2, 9, 4, 4, 2, 8, 128),
            vmem(9, 4, 4, 2, 8, 128),
            vmem(3, 4, 3, 4, 8, 128),
            vmem(3, 4, 3, 4, 8, 128),
            vmem(3, 3, 3, 4, 8, 128),
            vmem(3, 3, 3, 4, 8, 128),
            vmem(3, 4, 3, 8, 128),
            vmem(3, 4, 3, 8, 128),
            vmem(3, 3, 3, 8, 128),
            vmem(3, 3, 3, 8, 128),
            vmem(DEPTH, 9, 128),
            vmem(DEPTH - 1, 9, 128),
            vmem(9, 128),
            vmem(128, 128),
            vmem(128, 128),
            vmem(128, 128),
            vmem(128, 128),
            vmem(1, 128),
            vmem(PLANE - 1, 1, 128),
            vmem(2, PLANE, 2, 8, 128),
            vmem(2, PLANE, 2, 8, 128),
            vmem(2, PLANE, 2, 8, 128),
            vmem(2, PLANE, 2, 8, 128),
            vmem(2, 256, 256),
            vmem(2, PLANE, 2, 8, 128),
            vmem(2, PLANE, 2, 8, 128),
            vmem(128, 128),
            vmem(128, 128),
            pltpu.SemaphoreType.DMA,
            pltpu.SemaphoreType.DMA((9,)),
            pltpu.SemaphoreType.DMA((2,)),
            pltpu.SemaphoreType.DMA((6,)),
            pltpu.SemaphoreType.DMA((2,)),
            pltpu.SemaphoreType.DMA((6,)),
            pltpu.SemaphoreType.DMA,
            pltpu.SemaphoreType.DMA,
            pltpu.SemaphoreType.DMA((13,)),
            pltpu.SemaphoreType.DMA((13,)),
            pltpu.SemaphoreType.DMA((3,)),
        ],
        compiler_params=pltpu.CompilerParams(collective_id=0, has_side_effects=True, vmem_limit_bytes=63 * 2**20),
        name="step",
    )(inputs.reshape(CELLS, CHANNELS), cotangent.reshape(CELLS, CHANNELS), kernel_taps)
    return out.reshape(9, 4, 32)


def solution(mesh):
    torus = Mesh(mesh.devices.reshape(4, 8, 2, 2, 4), AXES)
    return jax.shard_map(
        body,
        mesh=torus,
        in_specs=(P(DP_INNER, None, None, None), P(DP_INNER, None, None, None), P(None, DP, INNER)),
        out_specs=P(None, DP, INNER),
        check_vma=False,
    )
```

```python
import functools
import math

import jax
import jax.numpy as jnp
from jax import lax
from jax.experimental import pallas as pl
from jax.experimental.pallas import tpu as pltpu
from jax.sharding import Mesh
from jax.sharding import PartitionSpec as P

AXES = ("dp_0", "dp_1", "dp_2", "inner_0", "inner_1")
INNER = ("inner_0", "inner_1")
DP = ("dp_0", "dp_1", "dp_2")
DP_INNER = DP + INNER
SIDE = 32
CHANNELS = 256
CELLS = SIDE * SIDE
STEP = 0.06 * math.sqrt(CHANNELS)
F32 = jnp.float32
BF16 = jnp.bfloat16
PLANE = 32
DEPTH = 16
CHUNKS = 3
MESH = pl.DeviceIdType.MESH
PEERS = sorted(
    [(dy, dc, dx) for dy in range(4) for dc in range(2) for dx in range(4) if dy or dc or dx],
    key=lambda m: -(min(m[0], 4 - m[0]) + min(m[2], 4 - m[2])),
)
STEPS = sorted(range(1, DEPTH), key=lambda d: -min(d, DEPTH - d))
COS = [math.cos(2.0 * math.pi * k / SIDE) for k in range(SIDE)]
SIN = [math.sin(2.0 * math.pi * k / SIDE) for k in range(SIDE)]


def swap_groups(parts):
    lane = lax.broadcasted_iota(jnp.int32, parts[0].shape, 1)
    low = lane < 64
    even = (lane & 32) == 0
    v0, v1, v2, v3 = parts
    w0 = jnp.where(low, v0, pltpu.roll(v2, 64, 1))
    w2 = jnp.where(low, pltpu.roll(v0, 64, 1), v2)
    w1 = jnp.where(low, v1, pltpu.roll(v3, 64, 1))
    w3 = jnp.where(low, pltpu.roll(v1, 64, 1), v3)
    u0 = jnp.where(even, w0, pltpu.roll(w1, 32, 1))
    u1 = jnp.where(even, pltpu.roll(w0, 96, 1), w1)
    u2 = jnp.where(even, w2, pltpu.roll(w3, 32, 1))
    u3 = jnp.where(even, pltpu.roll(w2, 96, 1), w3)
    return u0, u1, u2, u3


def halves(value):
    high = value.astype(BF16)
    low = (value - high.astype(F32)).astype(BF16)
    return high, low


def product(left, right):
    dot = functools.partial(jnp.dot, preferred_element_type=F32)
    return dot(left[0], right[0]) + (dot(left[0], right[1]) + dot(left[1], right[0]))


def kernel(x_hbm, ct_hbm, taps_hbm, out_ref, x_ref, ct_ref, taps_ref, xt, cb, go, gr, s0, s1, r0, r1, t0, t1, u0, u1, zs, zr, gs, as_t, ar_t,
           as_g, ar_g, nv, nr, ks_t, kr_t, ks_g, kr_g, mat, ao, ar, fs, fr, pair_send, pair_recv, a_send, a_recv,
           b_send, b_recv, c_send, c_recv, one_send, one_recv, load_sem, known):
    y = lax.axis_index("dp_0")
    zl = lax.axis_index("dp_1")
    c = lax.axis_index("dp_2")
    zh = lax.axis_index("inner_0")
    x = lax.axis_index("inner_1")
    z = zh * 8 + zl
    p = (y * 2 + c) * 4 + x

    ys = [y] + [lax.rem(y + d, 4) for d in range(1, 4)]
    xs = [x] + [lax.rem(x + d, 4) for d in range(1, 4)]
    cores = [c, 1 - c]
    depths = [z] + [lax.rem(z + d, DEPTH) for d in range(1, DEPTH)]

    def at_plane(peer):
        dy, dc, dx = peer
        return (ys[dy], zl, cores[dc], zh, xs[dx])

    def place(peer):
        dy, dc, dx = peer
        return (ys[dy] * 2 + cores[dc]) * 4 + xs[dx]

    def at_depth(d):
        return (y, lax.rem(depths[d], 8), c, lax.div(depths[d], 8), x)

    def send(src, dst, send_sem, recv_sem, device):
        pltpu.make_async_remote_copy(
            src_ref=src, dst_ref=dst, send_sem=send_sem, recv_sem=recv_sem, device_id=device, device_id_type=MESH
        ).start()

    def drain(ref, sem):
        pltpu.make_async_copy(ref, ref, sem).wait()

    pending = []

    def finish():
        for ref, sem in pending:
            drain(ref, sem)

    loads = [
        pltpu.make_async_copy(src, dst, load_sem.at[n])
        for n, (src, dst) in enumerate(((x_hbm, x_ref), (ct_hbm, ct_ref), (taps_hbm, taps_ref)))
    ]
    for load in loads:
        load.start()
    barrier = pltpu.get_barrier_semaphore()
    lines = [peer for peer in PEERS if sum(step != 0 for step in peer) == 1]
    for peer in lines:
        pl.semaphore_signal(barrier, inc=1, device_id=at_plane(peer), device_id_type=MESH)
    for d in (1, DEPTH - 1):
        pl.semaphore_signal(barrier, inc=1, device_id=at_depth(d), device_id_type=MESH)

    def tell(stage):
        for d in (2**stage, DEPTH - 2**stage):
            pl.semaphore_signal(known.at[stage], inc=1, device_id=at_depth(d), device_id_type=MESH)

    def learn(stage):
        pl.semaphore_wait(known.at[stage], 2)
        if stage < 2:
            tell(stage + 1)


    row = lax.broadcasted_iota(jnp.int32, (256, 256), 0)
    col = lax.broadcasted_iota(jnp.int32, (256, 256), 1)
    channel = (row & 192) + (row & 7) * 8 + ((row >> 5) & 1) * 4 + ((row >> 3) & 3)
    order = jnp.where(col == channel, 1.0, 0.0).astype(BF16)
    loads[0].wait()
    for k in range(4):
        xt[:, k * 256 : (k + 1) * 256] = lax.dot_general(
            order, x_ref[k * 256 : (k + 1) * 256, :], (((1,), (1,)), ((), ())), preferred_element_type=F32
        ).astype(BF16)
    loads[1].wait()
    for m in range(3):
        source = (row & 224) + ((row + (33 - m)) & 31)
        shift = jnp.where(col == source, 1.0, 0.0).astype(BF16)
        for k in range(4):
            rows = ct_ref[k * 256 : (k + 1) * 256, :]
            if m != 1:
                rows = jnp.dot(shift, rows, preferred_element_type=F32).astype(BF16)
            cb[m, 32 + k * 256 : 32 + (k + 1) * 256, :] = rows
        cb[m, 0:32, :] = cb[m, 1024:1056, :]
        cb[m, 1056:1088, :] = cb[m, 32:64, :]

    def depth_messages(block, dst):
        before, middle, after = [
            jnp.concatenate([block[3 * a + b : 3 * a + b + 1, :] for a in range(3)], axis=0) for b in range(3)
        ]
        both = after + before
        apart = after - before
        for w in range(DEPTH):
            if w == 0:
                upper, lower = middle + both, middle - both
            else:
                upper, lower = middle + COS[w] * both, -SIN[w] * apart
            dst[8 * w : 8 * w + 3, :] = upper
            dst[8 * w + 3 : 8 * w + 6, :] = lower
        return None

    def depth_send(src, dst, sem):
        for d in STEPS:
            slot = (4 - d) % DEPTH
            send(src.at[pl.ds(pl.multiple_of(depths[d] * 8, 8), 8)], dst.at[pl.ds(8 * slot, 8)],
                 one_send.at[sem], one_recv.at[sem + slot // 8], at_depth(d))
        dst[32:40, :] = src[pl.ds(pl.multiple_of(z * 8, 8), 8), :]
        pending.append((src.at[pl.ds(0, 120)], one_send.at[sem]))

    def depth_wait(dst, sem, half):
        drain(dst.at[pl.ds(0, 64 if half else 56)], one_recv.at[sem + half])

    def plane_messages(src, dst, half):
        parts = [src[pl.ds(64 * half + m, 8, stride=8), :] for m in range(6)]

        @pl.when(z != 0)
        def _():
            real_sum, real_gap = parts[2] + parts[0], parts[2] - parts[0]
            imag_sum, imag_gap = parts[5] + parts[3], parts[5] - parts[3]
            for k in range(17):
                upper, upper_gap = parts[1] + COS[k] * real_sum, SIN[k] * imag_gap
                lower, lower_gap = parts[4] + COS[k] * imag_sum, SIN[k] * real_gap
                dst[half, k, 0] = upper + upper_gap
                dst[half, k, 1] = lower - lower_gap
                if 0 < k < 16:
                    dst[half, 32 - k, 0] = upper - upper_gap
                    dst[half, 32 - k, 1] = lower + lower_gap

        @pl.when(z == 0)
        def _():
            for edge in range(2):
                first, mid, last = parts[3 * edge : 3 * edge + 3]
                total, gap = last + first, last - first
                dst[half, 16 * edge, 0] = mid + total
                dst[half, 16 * edge, 1] = mid - total
                for k in range(1, 16):
                    dst[half, 16 * edge + k, 0] = mid + COS[k] * total
                    dst[half, 16 * edge + k, 1] = -SIN[k] * gap

    def plane_send(src, dst, half, sem):
        for peer in PEERS:
            send(src.at[half, place(peer)], dst.at[half, p], one_send.at[sem + half], one_recv.at[sem + half], at_plane(peer))
        dst[half, p] = src[half, p]
        pending.append((src.at[half, pl.ds(0, PLANE - 1)], one_send.at[sem + half]))

    def plane_wait(dst, half, sem):
        drain(dst.at[half, pl.ds(0, PLANE - 1)], one_recv.at[sem + half])

    sublane = lax.broadcasted_iota(jnp.int32, (8, 128), 0)

    def turned(low, high, shift):
        rest = lax.rem(shift, 8)
        kept = (sublane >= rest) == (shift < 8)
        low, high = pltpu.roll(low, rest, 0), pltpu.roll(high, rest, 0)
        return jnp.where(kept, low, high), jnp.where(kept, high, low)

    as_t[...] = jnp.zeros_like(as_t)
    as_g[...] = jnp.zeros_like(as_g)
    fs[...] = jnp.zeros_like(fs)
    loads[2].wait()
    depth_messages(jnp.concatenate([taps_ref[:, i, :] for i in range(4)], axis=1), as_t)

    def chunk_out(ch):
        for t in range(3):
            drain(gr.at[3 * ch + t], pair_recv.at[3 * ch + t])
        for t in range(3):
            for yy in range(4):
                for xx in range(4):
                    s0[ch, xx, t, yy] = go[c, 3 * ch + t, yy, xx, 0] + gr[3 * ch + t, yy, xx, 0]
                    s1[ch, yy, t, xx] = go[c, 3 * ch + t, yy, xx, 1] + gr[3 * ch + t, yy, xx, 1]
        for d in (1, 3, 2):
            xx, yy = xs[d], ys[d]
            send(s0.at[ch, xx], r0.at[ch, d - 1], a_send.at[0], a_recv.at[ch], (y, zl, c, zh, xx))
            send(s1.at[ch, yy], r1.at[ch, d - 1], a_send.at[1], a_recv.at[3 + ch], (yy, zl, c, zh, x))

    def chunk_on(ch):
        drain(r0.at[ch], a_recv.at[ch])
        for t in range(3):
            for yy in range(4):
                t0[ch, yy, t] = (s0[ch, x, t, yy] + r0[ch, 0, t, yy]) + (r0[ch, 1, t, yy] + r0[ch, 2, t, yy])
        for d in (1, 3, 2):
            yy = ys[d]
            send(t0.at[ch, yy], u0.at[ch, d - 1], b_send.at[0], b_recv.at[ch], (yy, zl, c, zh, x))
        drain(r1.at[ch], a_recv.at[3 + ch])
        for t in range(3):
            for xx in range(4):
                t1[ch, xx, t] = (s1[ch, y, t, xx] + r1[ch, 0, t, xx]) + (r1[ch, 1, t, xx] + r1[ch, 2, t, xx])
        for d in (1, 3, 2):
            xx = xs[d]
            send(t1.at[ch, xx], u1.at[ch, d - 1], b_send.at[1], b_recv.at[3 + ch], (y, zl, c, zh, xx))

    def chunk_in(ch):
        drain(u0.at[ch], b_recv.at[ch])
        drain(u1.at[ch], b_recv.at[3 + ch])
        for t in range(3):
            first = (t0[ch, y, t] + u0[ch, 0, t]) + (u0[ch, 1, t] + u0[ch, 2, t])
            second = (t1[ch, x, t] + u1[ch, 0, t]) + (u1[ch, 1, t] + u1[ch, 2, t])
            for w in range(8):
                zs[w, 3 * ch + t : 3 * ch + t + 1, :] = first[w : w + 1, :]
                zs[8 + w, 3 * ch + t : 3 * ch + t + 1, :] = second[w : w + 1, :]

    for t in range(9):
        a, b = t // 3 - 1, t % 3
        grad = jnp.dot(xt[...], cb[b, 32 - 32 * a : 32 - 32 * a + CELLS, :], preferred_element_type=F32)
        for yc in range(8):
            for h in range(2):
                parts = [grad[yc * 32 + i * 8 : yc * 32 + i * 8 + 8, h * 128 : h * 128 + 128] for i in range(4)]
                for xx, part in enumerate(swap_groups(parts)):
                    go[yc % 2, t, yc // 2, xx, h] = part
        if t == 0:
            pl.semaphore_wait(barrier, len(lines) + 2)
            tell(0)
        send(go.at[1 - c, t], gr.at[t], pair_send, pair_recv.at[t], (y, zl, 1 - c, zh, x))
        if t == 4:
            chunk_out(0)
        if t == 7:
            chunk_out(1)
            learn(0)
    chunk_out(2)
    pending.append((go.at[0], pair_send))
    pending.append((r0, a_send.at[0]))
    pending.append((r1, a_send.at[1]))
    learn(1)
    for ch in range(CHUNKS):
        chunk_on(ch)
    pending.append((u0, b_send.at[0]))
    pending.append((u1, b_send.at[1]))
    learn(2)
    depth_send(as_t, ar_t, 0)
    for ch in range(CHUNKS):
        chunk_in(ch)

    for d in STEPS:
        send(zs.at[depths[d]], zr.at[d - 1], c_send, c_recv, at_depth(d))
    for half in range(2):
        depth_wait(ar_t, 0, half)
        plane_messages(ar_t, ks_t, half)
        plane_send(ks_t, kr_t, half, 4)
    drain(zr, c_recv)
    pending.append((zr, c_send))
    block = zs[z]
    for d in range(DEPTH - 1):
        block = block + zr[d]
    gs[...] = block
    depth_messages(gs[...], as_g)
    squares = jnp.sum(block * block, axis=0, keepdims=True)
    for w in range(DEPTH):
        as_g[8 * w + 6 : 8 * w + 7, :] = squares
    depth_send(as_g, ar_g, 2)
    depth_wait(ar_g, 2, 0)
    plane_messages(ar_g, ks_g, 0)
    plane_send(ks_g, kr_g, 0, 6)
    depth_wait(ar_g, 2, 1)
    plane_messages(ar_g, ks_g, 1)
    plane_send(ks_g, kr_g, 1, 6)
    nv[...] = jnp.sum(ar_g[pl.ds(6, DEPTH, stride=8), :], axis=0, keepdims=True)
    for d, peer in enumerate(PEERS):
        send(nv, nr.at[d], one_send.at[12], one_recv.at[12], at_plane(peer))
    pending.append((nr, one_send.at[12]))
    for half in range(2):
        plane_wait(kr_t, half, 4)
    drain(nr, one_recv.at[12])
    total = nv[...]
    for d in range(PLANE - 1):
        total = total + nr[d]
    norm = jnp.sqrt(jnp.sum(total, axis=1, keepdims=True))
    factor = jnp.broadcast_to(STEP / (norm + 1e-6), (8, 128))
    for half in range(2):
        plane_wait(kr_g, half, 6)

    onward = depths[12]
    for yc in range(8):
        for m in range(2):
            parts = []
            for xx in range(4):
                near, far = [kr_t[n, yc * 4 + xx, m] - factor * kr_g[n, yc * 4 + xx, m] for n in range(2)]
                parts.append(turned(near, far, onward))
            for h in range(2):
                for i, part in enumerate(swap_groups([pair[h] for pair in parts])):
                    mat[m, yc * 32 + i * 8 : yc * 32 + i * 8 + 8, h * 128 : h * 128 + 128] = part

    joint = jnp.where((z == 0) & (p % 16 == 0), 0.0, 1.0).astype(F32)
    for _ in range(2):
        real, imag = mat[0], mat[1]
        real_2, imag_2 = halves(real), halves(imag)
        real_t, imag_t = halves(real.T), halves(imag.T)
        first = product(real_t, real_2)
        second = product(imag_t, imag_2)
        cross = product(real_t, imag_2) - product(imag_t, real_2)
        eye = jnp.where(row == col, 1.5, 0.0)
        mix_first = halves(eye - 0.5 * (first + joint * second))
        mix_second = halves(eye - 0.5 * (second + joint * first))
        mix_cross = halves((-0.5 * joint) * cross)
        mat[0] = product(real_2, mix_first) - product(imag_2, mix_cross)
        mat[1] = product(real_2, mix_cross) + product(imag_2, mix_second)

    back = lax.rem(20 - z, DEPTH)
    for yc in range(8):
        for m in range(2):
            low, high = [
                swap_groups(
                    [mat[m, yc * 32 + i * 8 : yc * 32 + i * 8 + 8, h * 128 : h * 128 + 128] for i in range(4)]
                )
                for h in range(2)
            ]
            for xx in range(4):
                ao[0, yc * 4 + xx, m], ao[1, yc * 4 + xx, m] = turned(low[xx], high[xx], back)
    plane_send(ao, ar, 1, 8)
    plane_send(ao, ar, 0, 8)

    def summed(half, first, last, base):
        real_0 = imag_0 = real_c = real_s = imag_c = imag_s = jnp.zeros((8, 128), F32)
        for k in range(first, last):
            real, imag = ar[half, k, 0], ar[half, k, 1]
            ck, sk = COS[k - base], SIN[k - base]
            real_0, imag_0 = real_0 + real, imag_0 + imag
            real_c, real_s = real_c + ck * real, real_s + sk * real
            imag_c, imag_s = imag_c + ck * imag, imag_s + sk * imag
        return real_0, imag_0, real_c, real_s, imag_c, imag_s

    for half in (1, 0):
        plane_wait(ar, half, 8)

        @pl.when(z != 0)
        def _():
            real_0, imag_0, real_c, real_s, imag_c, imag_s = summed(half, 0, 32, 0)
            parts = (real_c + imag_s, real_0, real_c - imag_s, imag_c - real_s, imag_0, imag_c + real_s)
            for m, part in enumerate(parts):
                fs[pl.ds(64 * half + m, 8, stride=8), :] = 2.0 * part

        @pl.when(z == 0)
        def _():
            for edge in range(2):
                base = 16 * edge
                real_0, imag_0, real_c, real_s, imag_c, imag_s = summed(half, base + 1, base + 16, base)
                one, other = ar[half, base, 0], ar[half, base, 1]
                parts = (
                    2.0 * (real_c + imag_s) + (one - other),
                    2.0 * real_0 + (one + other),
                    2.0 * (real_c - imag_s) + (one - other),
                )
                for m, part in enumerate(parts):
                    fs[pl.ds(64 * half + 3 * edge + m, 8, stride=8), :] = part

        own = pl.ds(pl.multiple_of(z * 8, 8), 8)
        for d in STEPS:
            slot = (d + 4) % DEPTH
            if slot // 8 == half:
                send(fs.at[pl.ds(8 * slot, 8)], fr.at[own], one_send.at[10], one_recv.at[10], at_depth(d))
        if half == 0:
            fr[own, :] = fs[32:40, :]
    pending.append((fs.at[pl.ds(0, 120)], one_send.at[10]))
    drain(fr.at[pl.ds(0, 120)], one_recv.at[10])
    plain = fr[8:16, :]
    cosine = COS[1] * fr[8:16, :]
    sine = SIN[1] * fr[8:16, :]
    for w in range(2, DEPTH):
        tile = fr[8 * w : 8 * w + 8, :]
        plain, cosine, sine = plain + tile, cosine + COS[w] * tile, sine + SIN[w] * tile
    edge = fr[0:8, :]
    for a in range(3):
        first, last = edge[a : a + 1, :], edge[a + 3 : a + 4, :]
        even, odd = first + last, first - last
        out_ref[3 * a + 1 : 3 * a + 2, :] = (plain[a : a + 1, :] + even) * (1.0 / 64.0)
        out_ref[3 * a : 3 * a + 1, :] = (cosine[a : a + 1, :] + sine[a + 3 : a + 4, :] + odd) * (1.0 / 64.0)
        out_ref[3 * a + 2 : 3 * a + 3, :] = (cosine[a : a + 1, :] - sine[a + 3 : a + 4, :] + odd) * (1.0 / 64.0)

    finish()


def body(inputs, cotangent, kernel_taps):
    vmem = lambda *shape: pltpu.VMEM(shape, F32)
    out = pl.pallas_call(
        kernel,
        out_shape=jax.ShapeDtypeStruct((9, 128), F32),
        in_specs=[pl.BlockSpec(memory_space=pl.ANY)] * 3,
        out_specs=pl.BlockSpec(memory_space=pltpu.VMEM),
        scratch_shapes=[
            pltpu.VMEM((CELLS, CHANNELS), BF16),
            pltpu.VMEM((CELLS, CHANNELS), BF16),
            vmem(9, 4, 32),
            pltpu.VMEM((CHANNELS, CELLS), BF16),
            pltpu.VMEM((3, CELLS + 64, CHANNELS), BF16),
            vmem(2, 9, 4, 4, 2, 8, 128),
            vmem(9, 4, 4, 2, 8, 128),
            vmem(3, 4, 3, 4, 8, 128),
            vmem(3, 4, 3, 4, 8, 128),
            vmem(3, 3, 3, 4, 8, 128),
            vmem(3, 3, 3, 4, 8, 128),
            vmem(3, 4, 3, 8, 128),
            vmem(3, 4, 3, 8, 128),
            vmem(3, 3, 3, 8, 128),
            vmem(3, 3, 3, 8, 128),
            vmem(DEPTH, 9, 128),
            vmem(DEPTH - 1, 9, 128),
            vmem(9, 128),
            vmem(128, 128),
            vmem(128, 128),
            vmem(128, 128),
            vmem(128, 128),
            vmem(1, 128),
            vmem(PLANE - 1, 1, 128),
            vmem(2, PLANE, 2, 8, 128),
            vmem(2, PLANE, 2, 8, 128),
            vmem(2, PLANE, 2, 8, 128),
            vmem(2, PLANE, 2, 8, 128),
            vmem(2, 256, 256),
            vmem(2, PLANE, 2, 8, 128),
            vmem(2, PLANE, 2, 8, 128),
            vmem(128, 128),
            vmem(128, 128),
            pltpu.SemaphoreType.DMA,
            pltpu.SemaphoreType.DMA((9,)),
            pltpu.SemaphoreType.DMA((2,)),
            pltpu.SemaphoreType.DMA((6,)),
            pltpu.SemaphoreType.DMA((2,)),
            pltpu.SemaphoreType.DMA((6,)),
            pltpu.SemaphoreType.DMA,
            pltpu.SemaphoreType.DMA,
            pltpu.SemaphoreType.DMA((13,)),
            pltpu.SemaphoreType.DMA((13,)),
            pltpu.SemaphoreType.DMA((3,)),
            pltpu.SemaphoreType.REGULAR((3,)),
        ],
        compiler_params=pltpu.CompilerParams(collective_id=0, has_side_effects=True, vmem_limit_bytes=63 * 2**20),
        name="step",
    )(inputs.reshape(CELLS, CHANNELS), cotangent.reshape(CELLS, CHANNELS), kernel_taps)
    return out.reshape(9, 4, 32)


def solution(mesh):
    torus = Mesh(mesh.devices.reshape(4, 8, 2, 2, 4), AXES)
    return jax.shard_map(
        body,
        mesh=torus,
        in_specs=(P(DP_INNER, None, None, None), P(DP_INNER, None, None, None), P(None, DP, INNER)),
        out_specs=P(None, DP, INNER),
        check_vma=False,
    )
```

```python
import functools
import math

import jax
import jax.numpy as jnp
from jax import lax
from jax.experimental import pallas as pl
from jax.experimental.pallas import tpu as pltpu
from jax.sharding import Mesh
from jax.sharding import PartitionSpec as P

AXES = ("dp_0", "dp_1", "dp_2", "inner_0", "inner_1")
INNER = ("inner_0", "inner_1")
DP = ("dp_0", "dp_1", "dp_2")
DP_INNER = DP + INNER
SIDE = 32
CHANNELS = 256
CELLS = SIDE * SIDE
STEP = 0.06 * math.sqrt(CHANNELS)
F32 = jnp.float32
BF16 = jnp.bfloat16
PLANE = 32
DEPTH = 16
TAPS = (1, 4, 7, 0, 3, 6, 2, 5, 8)
GROUPS = ((0,), (1, 2), (3, 4, 5), (6, 7, 8))
FLOWS = (("x", 1, (0, 2, 4, 6, 8)), ("y", 1, (1, 3, 5, 7)), ("x", 0, (1, 3, 5, 7)), ("y", 0, (0, 2, 4, 6, 8)))
MESH = pl.DeviceIdType.MESH
PEERS = sorted(
    [(dy, dc, dx) for dy in range(4) for dc in range(2) for dx in range(4) if dy or dc or dx],
    key=lambda m: -(min(m[0], 4 - m[0]) + min(m[2], 4 - m[2])),
)
STEPS = sorted(range(1, DEPTH), key=lambda d: -min(d, DEPTH - d))
COS = [math.cos(2.0 * math.pi * k / SIDE) for k in range(SIDE)]
SIN = [math.sin(2.0 * math.pi * k / SIDE) for k in range(SIDE)]


def swap_groups(parts):
    lane = lax.broadcasted_iota(jnp.int32, parts[0].shape, 1)
    low = lane < 64
    even = (lane & 32) == 0
    v0, v1, v2, v3 = parts
    w0 = jnp.where(low, v0, pltpu.roll(v2, 64, 1))
    w2 = jnp.where(low, pltpu.roll(v0, 64, 1), v2)
    w1 = jnp.where(low, v1, pltpu.roll(v3, 64, 1))
    w3 = jnp.where(low, pltpu.roll(v1, 64, 1), v3)
    u0 = jnp.where(even, w0, pltpu.roll(w1, 32, 1))
    u1 = jnp.where(even, pltpu.roll(w0, 96, 1), w1)
    u2 = jnp.where(even, w2, pltpu.roll(w3, 32, 1))
    u3 = jnp.where(even, pltpu.roll(w2, 96, 1), w3)
    return u0, u1, u2, u3


def halves(value):
    high = value.astype(BF16)
    low = (value - high.astype(F32)).astype(BF16)
    return high, low


def product(left, right):
    dot = functools.partial(jnp.dot, preferred_element_type=F32)
    return dot(left[0], right[0]) + (dot(left[0], right[1]) + dot(left[1], right[0]))


def kernel(x_hbm, ct_hbm, taps_hbm, out_ref, x_ref, ct_ref, taps_ref, xt, cb, go, gr, s0, s1, s2, s3, r0, r1, r2, r3, t0, t1, t2, t3, u0, u1, u2, u3, zs, zr, gs, as_t, ar_t,
           as_g, ar_g, nv, nr, ks_t, kr_t, ks_g, kr_g, mat, ao, ar, fs, fr, pair_send, pair_recv, a_send, a_recv,
           b_send, b_recv, c_send, c_recv, one_send, one_recv, load_sem, known):
    y = lax.axis_index("dp_0")
    zl = lax.axis_index("dp_1")
    c = lax.axis_index("dp_2")
    zh = lax.axis_index("inner_0")
    x = lax.axis_index("inner_1")
    z = zh * 8 + zl
    p = (y * 2 + c) * 4 + x

    ys = [y] + [lax.rem(y + d, 4) for d in range(1, 4)]
    xs = [x] + [lax.rem(x + d, 4) for d in range(1, 4)]
    cores = [c, 1 - c]
    depths = [z] + [lax.rem(z + d, DEPTH) for d in range(1, DEPTH)]

    def at_plane(peer):
        dy, dc, dx = peer
        return (ys[dy], zl, cores[dc], zh, xs[dx])

    def place(peer):
        dy, dc, dx = peer
        return (ys[dy] * 2 + cores[dc]) * 4 + xs[dx]

    def at_depth(d):
        return (y, lax.rem(depths[d], 8), c, lax.div(depths[d], 8), x)

    def send(src, dst, send_sem, recv_sem, device):
        pltpu.make_async_remote_copy(
            src_ref=src, dst_ref=dst, send_sem=send_sem, recv_sem=recv_sem, device_id=device, device_id_type=MESH
        ).start()

    def drain(ref, sem):
        pltpu.make_async_copy(ref, ref, sem).wait()

    pending = []

    def finish():
        for ref, sem in pending:
            drain(ref, sem)

    loads = [
        pltpu.make_async_copy(src, dst, load_sem.at[n])
        for n, (src, dst) in enumerate(((x_hbm, x_ref), (ct_hbm, ct_ref), (taps_hbm, taps_ref)))
    ]
    for load in loads:
        load.start()
    barrier = pltpu.get_barrier_semaphore()
    lines = [peer for peer in PEERS if sum(step != 0 for step in peer) == 1]
    for peer in lines:
        pl.semaphore_signal(barrier, inc=1, device_id=at_plane(peer), device_id_type=MESH)
    for d in (1, DEPTH - 1):
        pl.semaphore_signal(barrier, inc=1, device_id=at_depth(d), device_id_type=MESH)

    def tell(stage):
        for d in (2**stage, DEPTH - 2**stage):
            pl.semaphore_signal(known.at[stage], inc=1, device_id=at_depth(d), device_id_type=MESH)

    def learn(stage):
        pl.semaphore_wait(known.at[stage], 2)
        if stage < 2:
            tell(stage + 1)


    row = lax.broadcasted_iota(jnp.int32, (256, 256), 0)
    col = lax.broadcasted_iota(jnp.int32, (256, 256), 1)
    channel = (row & 192) + (row & 7) * 8 + ((row >> 5) & 1) * 4 + ((row >> 3) & 3)
    order = jnp.where(col == channel, 1.0, 0.0).astype(BF16)
    loads[0].wait()
    for k in range(4):
        xt[:, k * 256 : (k + 1) * 256] = lax.dot_general(
            order, x_ref[k * 256 : (k + 1) * 256, :], (((1,), (1,)), ((), ())), preferred_element_type=F32
        ).astype(BF16)
    loads[1].wait()

    def moved(m):
        source = (row & 224) + ((row + (33 - m)) & 31)
        shift = jnp.where(col == source, 1.0, 0.0).astype(BF16)
        for k in range(4):
            rows = ct_ref[k * 256 : (k + 1) * 256, :]
            if m != 1:
                rows = jnp.dot(shift, rows, preferred_element_type=F32).astype(BF16)
            cb[m, 32 + k * 256 : 32 + (k + 1) * 256, :] = rows
        cb[m, 0:32, :] = cb[m, 1024:1056, :]
        cb[m, 1056:1088, :] = cb[m, 32:64, :]

    def depth_messages(block, dst):
        before, middle, after = [
            jnp.concatenate([block[3 * a + b : 3 * a + b + 1, :] for a in range(3)], axis=0) for b in range(3)
        ]
        both = after + before
        apart = after - before
        for w in range(DEPTH):
            if w == 0:
                upper, lower = middle + both, middle - both
            else:
                upper, lower = middle + COS[w] * both, -SIN[w] * apart
            dst[8 * w : 8 * w + 3, :] = upper
            dst[8 * w + 3 : 8 * w + 6, :] = lower
        return None

    def depth_send(src, dst, sem):
        for d in STEPS:
            slot = (4 - d) % DEPTH
            send(src.at[pl.ds(pl.multiple_of(depths[d] * 8, 8), 8)], dst.at[pl.ds(8 * slot, 8)],
                 one_send.at[sem], one_recv.at[sem + slot // 8], at_depth(d))
        dst[32:40, :] = src[pl.ds(pl.multiple_of(z * 8, 8), 8), :]
        pending.append((src.at[pl.ds(0, 120)], one_send.at[sem]))

    def depth_wait(dst, sem, half):
        drain(dst.at[pl.ds(0, 64 if half else 56)], one_recv.at[sem + half])

    def plane_messages(src, dst, half):
        parts = [src[pl.ds(64 * half + m, 8, stride=8), :] for m in range(6)]

        @pl.when(z != 0)
        def _():
            real_sum, real_gap = parts[2] + parts[0], parts[2] - parts[0]
            imag_sum, imag_gap = parts[5] + parts[3], parts[5] - parts[3]
            for k in range(17):
                upper, upper_gap = parts[1] + COS[k] * real_sum, SIN[k] * imag_gap
                lower, lower_gap = parts[4] + COS[k] * imag_sum, SIN[k] * real_gap
                dst[half, k, 0] = upper + upper_gap
                dst[half, k, 1] = lower - lower_gap
                if 0 < k < 16:
                    dst[half, 32 - k, 0] = upper - upper_gap
                    dst[half, 32 - k, 1] = lower + lower_gap

        @pl.when(z == 0)
        def _():
            for edge in range(2):
                first, mid, last = parts[3 * edge : 3 * edge + 3]
                total, gap = last + first, last - first
                dst[half, 16 * edge, 0] = mid + total
                dst[half, 16 * edge, 1] = mid - total
                for k in range(1, 16):
                    dst[half, 16 * edge + k, 0] = mid + COS[k] * total
                    dst[half, 16 * edge + k, 1] = -SIN[k] * gap

    def plane_send(src, dst, half, sem):
        for peer in PEERS:
            send(src.at[half, place(peer)], dst.at[half, p], one_send.at[sem + half], one_recv.at[sem + half], at_plane(peer))
        dst[half, p] = src[half, p]
        pending.append((src.at[half, pl.ds(0, PLANE - 1)], one_send.at[sem + half]))

    def plane_wait(dst, half, sem):
        drain(dst.at[half, pl.ds(0, PLANE - 1)], one_recv.at[sem + half])

    sublane = lax.broadcasted_iota(jnp.int32, (8, 128), 0)

    def turned(low, high, shift):
        rest = lax.rem(shift, 8)
        kept = (sublane >= rest) == (shift < 8)
        low, high = pltpu.roll(low, rest, 0), pltpu.roll(high, rest, 0)
        return jnp.where(kept, low, high), jnp.where(kept, high, low)

    sums, heard, lines_2, heard_2 = (s0, s1, s2, s3), (r0, r1, r2, r3), (t0, t1, t2, t3), (u0, u1, u2, u3)
    along = {"x": (xs, lambda v: (y, zl, c, zh, v)), "y": (ys, lambda v: (v, zl, c, zh, x))}

    def chunk_out(ch):
        for n in GROUPS[ch]:
            drain(gr.at[n], pair_recv.at[n])
        for f, (axis, half, places) in enumerate(FLOWS):
            ready = [k for k, n in enumerate(places) if n in GROUPS[ch]]
            for k in ready:
                n = places[k]
                for yy in range(4):
                    for xx in range(4):
                        to, other = (xx, yy) if axis == "x" else (yy, xx)
                        sums[f][to, k, other] = go[c, n, yy, xx, half] + gr[n, yy, xx, half]
            if ready and (half or ch == 0):
                flow_out(f, ready[0], len(ready))

    def flow_out(f, start, count):
        where, device = along[FLOWS[f][0]]
        part = pl.ds(start, count)
        for d in (2, 1, 3):
            send(sums[f].at[where[d], part], heard[f].at[d - 1, part], a_send.at[f], a_recv.at[f], device(where[d]))

    def flow_on(f):
        axis, _, places = FLOWS[f]
        mine = x if axis == "x" else y
        where, device = along["y" if axis == "x" else "x"]
        drain(heard[f], a_recv.at[f])
        for k in range(len(places)):
            for o in range(4):
                lines_2[f][o, k] = (sums[f][mine, k, o] + heard[f][0, k, o]) + (heard[f][1, k, o] + heard[f][2, k, o])
        for d in (2, 1, 3):
            send(lines_2[f].at[where[d]], heard_2[f].at[d - 1], b_send.at[f], b_recv.at[f], device(where[d]))
        pending.append((heard[f], a_send.at[f]))
        pending.append((heard_2[f], b_send.at[f]))

    def flow_in(f):
        axis, half, places = FLOWS[f]
        mine = y if axis == "x" else x
        drain(heard_2[f], b_recv.at[f])
        for k, n in enumerate(places):
            tile = (lines_2[f][mine, k] + heard_2[f][0, k]) + (heard_2[f][1, k] + heard_2[f][2, k])
            for w in range(8):
                zs[8 * half + w, TAPS[n] : TAPS[n] + 1, :] = tile[w : w + 1, :]

    def depth_sum(half):
        for d in STEPS:
            slot = (d + 4) % DEPTH
            if slot // 8 == half:
                send(zs.at[slot], zr.at[d - 1], c_send, c_recv, at_depth(d))

    back = lax.rem(20 - z, DEPTH)
    moved(1)
    for n, t in enumerate(TAPS):
        a, b = t // 3 - 1, t % 3
        grad = jnp.dot(xt[...], cb[b, 32 - 32 * a : 32 - 32 * a + CELLS, :], preferred_element_type=F32)
        for yc in range(8):
            low, high = [
                swap_groups(
                    [grad[yc * 32 + i * 8 : yc * 32 + i * 8 + 8, h * 128 : h * 128 + 128] for i in range(4)]
                )
                for h in range(2)
            ]
            for xx in range(4):
                near, far = turned(low[xx], high[xx], back)
                go[yc % 2, n, yc // 2, xx, 0] = near
                go[yc % 2, n, yc // 2, xx, 1] = far
        if n == 0:
            pl.semaphore_wait(barrier, len(lines) + 2)
            tell(0)
        send(go.at[1 - c, n], gr.at[n], pair_send, pair_recv.at[n], (y, zl, 1 - c, zh, x))
        if n == 2:
            moved(0)
            chunk_out(0)
        if n == 3:
            chunk_out(1)
        if n == 5:
            moved(2)
        if n == 6:
            chunk_out(2)
            learn(0)
    chunk_out(3)
    flow_out(2, 0, 4)
    flow_out(3, 1, 4)
    pending.append((go.at[0], pair_send))
    as_t[...] = jnp.zeros_like(as_t)
    as_g[...] = jnp.zeros_like(as_g)
    fs[...] = jnp.zeros_like(fs)
    loads[2].wait()
    depth_messages(jnp.concatenate([taps_ref[:, i, :] for i in range(4)], axis=1), as_t)

    learn(1)
    flow_on(0)
    flow_on(1)
    learn(2)
    depth_send(as_t, ar_t, 0)
    flow_on(2)
    flow_on(3)
    flow_in(0)
    flow_in(1)
    depth_sum(1)
    flow_in(2)
    flow_in(3)
    depth_sum(0)

    for half in range(2):
        depth_wait(ar_t, 0, half)
        plane_messages(ar_t, ks_t, half)
        plane_send(ks_t, kr_t, half, 4)
    drain(zr, c_recv)
    pending.append((zr, c_send))
    block = zs[4]
    for d in range(DEPTH - 1):
        block = block + zr[d]
    gs[...] = block
    depth_messages(gs[...], as_g)
    squares = jnp.sum(block * block, axis=0, keepdims=True)
    for w in range(DEPTH):
        as_g[8 * w + 6 : 8 * w + 7, :] = squares
    depth_send(as_g, ar_g, 2)
    depth_wait(ar_g, 2, 0)
    plane_messages(ar_g, ks_g, 0)
    plane_send(ks_g, kr_g, 0, 6)
    depth_wait(ar_g, 2, 1)
    plane_messages(ar_g, ks_g, 1)
    plane_send(ks_g, kr_g, 1, 6)
    nv[...] = jnp.sum(ar_g[pl.ds(6, DEPTH, stride=8), :], axis=0, keepdims=True)
    for d, peer in enumerate(PEERS):
        send(nv, nr.at[d], one_send.at[12], one_recv.at[12], at_plane(peer))
    pending.append((nr, one_send.at[12]))
    for half in range(2):
        plane_wait(kr_t, half, 4)
    drain(nr, one_recv.at[12])
    total = nv[...]
    for d in range(PLANE - 1):
        total = total + nr[d]
    norm = jnp.sqrt(jnp.sum(total, axis=1, keepdims=True))
    factor = jnp.broadcast_to(STEP / (norm + 1e-6), (8, 128))
    for half in range(2):
        plane_wait(kr_g, half, 6)

    onward = depths[12]
    for yc in range(8):
        for m in range(2):
            parts = []
            for xx in range(4):
                near, far = [kr_t[n, yc * 4 + xx, m] - factor * kr_g[n, yc * 4 + xx, m] for n in range(2)]
                parts.append(turned(near, far, onward))
            for h in range(2):
                for i, part in enumerate(swap_groups([pair[h] for pair in parts])):
                    mat[m, yc * 32 + i * 8 : yc * 32 + i * 8 + 8, h * 128 : h * 128 + 128] = part

    joint = jnp.where((z == 0) & (p % 16 == 0), 0.0, 1.0).astype(F32)
    for _ in range(2):
        real, imag = mat[0], mat[1]
        real_2, imag_2 = halves(real), halves(imag)
        real_t, imag_t = halves(real.T), halves(imag.T)
        first = product(real_t, real_2)
        second = product(imag_t, imag_2)
        cross = product(real_t, imag_2) - product(imag_t, real_2)
        eye = jnp.where(row == col, 1.5, 0.0)
        mix_first = halves(eye - 0.5 * (first + joint * second))
        mix_second = halves(eye - 0.5 * (second + joint * first))
        mix_cross = halves((-0.5 * joint) * cross)
        mat[0] = product(real_2, mix_first) - product(imag_2, mix_cross)
        mat[1] = product(real_2, mix_cross) + product(imag_2, mix_second)

    for yc in range(8):
        for m in range(2):
            low, high = [
                swap_groups(
                    [mat[m, yc * 32 + i * 8 : yc * 32 + i * 8 + 8, h * 128 : h * 128 + 128] for i in range(4)]
                )
                for h in range(2)
            ]
            for xx in range(4):
                ao[0, yc * 4 + xx, m], ao[1, yc * 4 + xx, m] = turned(low[xx], high[xx], back)
    plane_send(ao, ar, 1, 8)
    plane_send(ao, ar, 0, 8)

    def summed(half, first, last, base):
        real_0 = imag_0 = real_c = real_s = imag_c = imag_s = jnp.zeros((8, 128), F32)
        for k in range(first, last):
            real, imag = ar[half, k, 0], ar[half, k, 1]
            ck, sk = COS[k - base], SIN[k - base]
            real_0, imag_0 = real_0 + real, imag_0 + imag
            real_c, real_s = real_c + ck * real, real_s + sk * real
            imag_c, imag_s = imag_c + ck * imag, imag_s + sk * imag
        return real_0, imag_0, real_c, real_s, imag_c, imag_s

    for half in (1, 0):
        plane_wait(ar, half, 8)

        @pl.when(z != 0)
        def _():
            real_0, imag_0, real_c, real_s, imag_c, imag_s = summed(half, 0, 32, 0)
            parts = (real_c + imag_s, real_0, real_c - imag_s, imag_c - real_s, imag_0, imag_c + real_s)
            for m, part in enumerate(parts):
                fs[pl.ds(64 * half + m, 8, stride=8), :] = 2.0 * part

        @pl.when(z == 0)
        def _():
            for edge in range(2):
                base = 16 * edge
                real_0, imag_0, real_c, real_s, imag_c, imag_s = summed(half, base + 1, base + 16, base)
                one, other = ar[half, base, 0], ar[half, base, 1]
                parts = (
                    2.0 * (real_c + imag_s) + (one - other),
                    2.0 * real_0 + (one + other),
                    2.0 * (real_c - imag_s) + (one - other),
                )
                for m, part in enumerate(parts):
                    fs[pl.ds(64 * half + 3 * edge + m, 8, stride=8), :] = part

        own = pl.ds(pl.multiple_of(z * 8, 8), 8)
        for d in STEPS:
            slot = (d + 4) % DEPTH
            if slot // 8 == half:
                send(fs.at[pl.ds(8 * slot, 8)], fr.at[own], one_send.at[10], one_recv.at[10], at_depth(d))
        if half == 0:
            fr[own, :] = fs[32:40, :]
    pending.append((fs.at[pl.ds(0, 120)], one_send.at[10]))
    drain(fr.at[pl.ds(0, 120)], one_recv.at[10])
    plain = fr[8:16, :]
    cosine = COS[1] * fr[8:16, :]
    sine = SIN[1] * fr[8:16, :]
    for w in range(2, DEPTH):
        tile = fr[8 * w : 8 * w + 8, :]
        plain, cosine, sine = plain + tile, cosine + COS[w] * tile, sine + SIN[w] * tile
    edge = fr[0:8, :]
    for a in range(3):
        first, last = edge[a : a + 1, :], edge[a + 3 : a + 4, :]
        even, odd = first + last, first - last
        out_ref[3 * a + 1 : 3 * a + 2, :] = (plain[a : a + 1, :] + even) * (1.0 / 64.0)
        out_ref[3 * a : 3 * a + 1, :] = (cosine[a : a + 1, :] + sine[a + 3 : a + 4, :] + odd) * (1.0 / 64.0)
        out_ref[3 * a + 2 : 3 * a + 3, :] = (cosine[a : a + 1, :] - sine[a + 3 : a + 4, :] + odd) * (1.0 / 64.0)

    finish()


def body(inputs, cotangent, kernel_taps):
    vmem = lambda *shape: pltpu.VMEM(shape, F32)
    out = pl.pallas_call(
        kernel,
        out_shape=jax.ShapeDtypeStruct((9, 128), F32),
        in_specs=[pl.BlockSpec(memory_space=pl.ANY)] * 3,
        out_specs=pl.BlockSpec(memory_space=pltpu.VMEM),
        scratch_shapes=[
            pltpu.VMEM((CELLS, CHANNELS), BF16),
            pltpu.VMEM((CELLS, CHANNELS), BF16),
            vmem(9, 4, 32),
            pltpu.VMEM((CHANNELS, CELLS), BF16),
            pltpu.VMEM((3, CELLS + 64, CHANNELS), BF16),
            vmem(2, 9, 4, 4, 2, 8, 128),
            vmem(9, 4, 4, 2, 8, 128),
            *[vmem(4, len(places), 4, 8, 128) for _, _, places in FLOWS],
            *[vmem(3, len(places), 4, 8, 128) for _, _, places in FLOWS],
            *[vmem(4, len(places), 8, 128) for _, _, places in FLOWS],
            *[vmem(3, len(places), 8, 128) for _, _, places in FLOWS],
            vmem(DEPTH, 9, 128),
            vmem(DEPTH - 1, 9, 128),
            vmem(9, 128),
            vmem(128, 128),
            vmem(128, 128),
            vmem(128, 128),
            vmem(128, 128),
            vmem(1, 128),
            vmem(PLANE - 1, 1, 128),
            vmem(2, PLANE, 2, 8, 128),
            vmem(2, PLANE, 2, 8, 128),
            vmem(2, PLANE, 2, 8, 128),
            vmem(2, PLANE, 2, 8, 128),
            vmem(2, 256, 256),
            vmem(2, PLANE, 2, 8, 128),
            vmem(2, PLANE, 2, 8, 128),
            vmem(128, 128),
            vmem(128, 128),
            pltpu.SemaphoreType.DMA,
            pltpu.SemaphoreType.DMA((9,)),
            pltpu.SemaphoreType.DMA((4,)),
            pltpu.SemaphoreType.DMA((4,)),
            pltpu.SemaphoreType.DMA((4,)),
            pltpu.SemaphoreType.DMA((4,)),
            pltpu.SemaphoreType.DMA,
            pltpu.SemaphoreType.DMA,
            pltpu.SemaphoreType.DMA((13,)),
            pltpu.SemaphoreType.DMA((13,)),
            pltpu.SemaphoreType.DMA((3,)),
            pltpu.SemaphoreType.REGULAR((3,)),
        ],
        compiler_params=pltpu.CompilerParams(collective_id=0, has_side_effects=True, vmem_limit_bytes=63 * 2**20),
        name="step",
    )(inputs.reshape(CELLS, CHANNELS), cotangent.reshape(CELLS, CHANNELS), kernel_taps)
    return out.reshape(9, 4, 32)


def solution(mesh):
    torus = Mesh(mesh.devices.reshape(4, 8, 2, 2, 4), AXES)
    return jax.shard_map(
        body,
        mesh=torus,
        in_specs=(P(DP_INNER, None, None, None), P(DP_INNER, None, None, None), P(None, DP, INNER)),
        out_specs=P(None, DP, INNER),
        check_vma=False,
    )
```
